32 devices in a mesh: row: 8 (over y, x, core), col: 4 (over z).
Axes of the slice: x: 2, y: 2, z: 4, core: 2. Of those that a mesh axis runs over, the one named last changes fastest.
Arguments:
- query_proj: bfloat16 [192, 192, 128], P('row', 'col'), may hold values from -8 to 8
- key_proj: bfloat16 [192, 192, 128], P('row', 'col'), may hold values from -8 to 8
- value_proj: bfloat16 [192, 192, 128], P('row', 'col'), may hold values from -6 to 6
- pair_bias: bfloat16 [4, 192, 192], P(None, 'col', 'row'), may hold values from -9 to 9
- pair_mask: int32 [192, 192], P('row', 'col'), may hold values 0 or 1
- grad_out: bfloat16 [192, 192, 128], P('row', 'col'), may hold values from -18 to 18
Outputs:
- grad_query: bfloat16 [192, 192, 128], P('row', 'col')
- grad_key: bfloat16 [192, 192, 128], P('row', 'col')
- grad_value: bfloat16 [192, 192, 128], P('row', 'col')
- grad_bias: float32 [4, 192, 192], P(None, 'col', 'row')
The draws below stay inside these ranges and needn't reach their ends.
All inputs are finite; a program needn't handle non-finite values. No bound on the sum of `pair_mask` on one device may be relied on, other than what follows from the above.
Results may differ from the reference program's by a relative error of at most 0.0096.
Values may be sent and summed in bfloat16 or wider, within the bound.
A program may use at most 128 MiB of HBM per device.

```python
import math
import jax
import jax.numpy as jnp
from jax import lax

HEADS = 4
HEAD_DIM = 32
RESIDUES = 192
CHANNELS = 128


def field_draw(key):
    return jnp.clip(jax.random.normal(key, (RESIDUES, RESIDUES, CHANNELS), jnp.float32), -6.0, 6.0)


def draw_query_proj(key, part):
    values_drawn = field_draw(jax.random.fold_in(key, 1))
    return values_drawn.astype(jnp.bfloat16)


def draw_key_proj(key, part):
    values_drawn = field_draw(jax.random.fold_in(key, 2))
    return values_drawn.astype(jnp.bfloat16)


def place_ends(values, own_key, least, top_value):
    dims = values.shape
    index_at = [jax.random.randint(jax.random.fold_in(own_key, axis), (), 0, dims[axis]) for axis in range(len(dims))]
    values = values.at[tuple(index_at)].set(least)
    longest = dims.index(max(dims))
    index_at[longest] = (index_at[longest] + 1) % dims[longest]
    return values.at[tuple(index_at)].set(top_value)


def steps_of(own_key, extent, split, least, largest):
    loudness, own = 1.0, jax.random.fold_in(own_key, 6)
    for dim, shards_of in split:
        heights = jnp.exp(jax.random.uniform(jax.random.fold_in(own, dim), (shards_of,), jnp.float32, least / len(split), largest / len(split)))
        loudness = loudness * jnp.repeat(heights, extent[dim] // shards_of).reshape([-1 if axis == dim else 1 for axis in range(len(extent))])
    return loudness


def noise(key, shape, deviation, limit, cuts=(), held_as=jnp.bfloat16):
    level = steps_of(key, shape, cuts, -0.22, 0.18) if cuts else 1.0
    result = jax.random.normal(key, shape, jnp.float32) * deviation * level
    return jnp.minimum(jnp.maximum(result, -limit), limit).astype(held_as)


def setup_inputs(seed: int = 0) -> dict:
    seeds = jax.random.split(jax.random.key(seed), 7)
    query_proj = draw_query_proj(jax.random.fold_in(seeds[6], 71), 0)
    key_proj = draw_key_proj(jax.random.fold_in(seeds[6], 71), 0)
    value_proj = noise(seeds[2], (RESIDUES, RESIDUES, CHANNELS), 1.0, 6.0, ((0, 8), (1, 4)))
    pair_bias = noise(seeds[3], (HEADS, RESIDUES, RESIDUES), 1.5, 9.0, ((1, 4), (2, 8)))
    pair_mask = place_ends((jax.random.randint(seeds[4], (RESIDUES, RESIDUES), 0, 4) < 3).astype(jnp.int32), jax.random.fold_in(seeds[4], 1), 0, 1)
    grad_out = noise(seeds[5], (RESIDUES, RESIDUES, CHANNELS), 3.0, 18.0, ((0, 8), (1, 4)))
    return {"query_proj": query_proj, "key_proj": key_proj, "value_proj": value_proj, "pair_bias": pair_bias, "pair_mask": pair_mask, "grad_out": grad_out}


def block_grads(queries, keys_all, values_all, grads, mask_all, bias_full):
    block_rows, query_count, channel_count = queries.shape
    key_count = keys_all.shape[1]
    scale = 1.0 / math.sqrt(HEAD_DIM)
    query_heads = queries.astype(jnp.float32).reshape(block_rows, query_count, HEADS, HEAD_DIM)
    key_heads = keys_all.astype(jnp.float32).reshape(block_rows, key_count, HEADS, HEAD_DIM)
    value_heads = values_all.astype(jnp.float32).reshape(block_rows, key_count, HEADS, HEAD_DIM)
    grad_heads = grads.astype(jnp.float32).reshape(block_rows, query_count, HEADS, HEAD_DIM)
    masked = 1000000000.0 * (mask_all.astype(jnp.float32) - 1.0)
    scores = jnp.einsum('bjhd,bkhd->bhjk', query_heads, key_heads) * scale
    scores = scores + bias_full.astype(jnp.float32)[None] + masked[:, None, None, :]
    top_score = lax.optimization_barrier(jnp.max(scores, axis=-1, keepdims=True))
    weights = jnp.exp(scores - top_score)
    attn_probs = weights / lax.optimization_barrier(jnp.sum(weights, axis=-1, keepdims=True))
    attn_low = attn_probs.astype(jnp.bfloat16).astype(jnp.float32)
    attended = jnp.einsum('bhjk,bkhd->bjhd', attn_low, value_heads)
    row_delta = lax.optimization_barrier(jnp.sum(grad_heads * attended, axis=-1))
    grad_probs = jnp.einsum('bjhd,bkhd->bhjk', grad_heads, value_heads)
    grad_scores = attn_probs * (grad_probs - jnp.transpose(row_delta, (0, 2, 1))[..., None])
    scores_low = grad_scores.astype(jnp.bfloat16).astype(jnp.float32)
    grad_queries = jnp.einsum('bhjk,bkhd->bjhd', scores_low, key_heads) * scale
    grad_keys = jnp.einsum('bhjk,bjhd->bkhd', scores_low, query_heads) * scale
    grad_values = jnp.einsum('bhjk,bjhd->bkhd', attn_low, grad_heads)
    bias_grad = lax.optimization_barrier(jnp.sum(grad_scores, axis=0))
    return (grad_queries.reshape(block_rows, query_count, channel_count), grad_keys.reshape(block_rows, key_count, channel_count), grad_values.reshape(block_rows, key_count, channel_count), bias_grad)

def reference(query_proj, key_proj, value_proj, pair_bias, pair_mask, grad_out):
    block_rows = math.gcd(RESIDUES, 8)
    steps_count = RESIDUES // block_rows

    def split_rows(array):
        return array.reshape((steps_count, block_rows) + array.shape[1:])

    def one_block(bias_sum, pieces):
        grad_queries, grad_keys, grad_values, bias_grad = block_grads(pieces[0], pieces[1], pieces[2], pieces[3], pieces[4], pair_bias)
        return (bias_sum + bias_grad, (grad_queries.astype(jnp.bfloat16), grad_keys.astype(jnp.bfloat16), grad_values.astype(jnp.bfloat16)))
    start_sum = jnp.zeros((HEADS, RESIDUES, RESIDUES), jnp.float32)
    bias_sum, stacked = lax.scan(one_block, start_sum, (split_rows(query_proj), split_rows(key_proj), split_rows(value_proj), split_rows(grad_out), split_rows(pair_mask)))
    full_shape = (RESIDUES, RESIDUES, CHANNELS)
    return (stacked[0].reshape(full_shape), stacked[1].reshape(full_shape), stacked[2].reshape(full_shape), bias_sum)
```

```python
import functools
import math

import jax
import jax.numpy as jnp
from jax import lax
from jax.experimental import pallas as pl
from jax.experimental.pallas import tpu as pltpu
from jax.sharding import PartitionSpec as P

HEADS = 4
HEAD_DIM = 32


def block_grads(queries, keys_all, values_all, grads, mask_all, bias_full):
    block_rows, query_count, channel_count = queries.shape
    key_count = keys_all.shape[1]
    scale = 1.0 / math.sqrt(HEAD_DIM)
    query_heads = queries.reshape(block_rows, query_count, HEADS, HEAD_DIM)
    key_heads = keys_all.reshape(block_rows, key_count, HEADS, HEAD_DIM)
    value_heads = values_all.reshape(block_rows, key_count, HEADS, HEAD_DIM)
    grad_heads = grads.reshape(block_rows, query_count, HEADS, HEAD_DIM)
    masked = 1000000000.0 * (mask_all.astype(jnp.float32) - 1.0)
    scores = (
        jnp.einsum("bjhd,bkhd->bhjk", query_heads, key_heads, preferred_element_type=jnp.float32)
        * scale
    )
    scores = scores + bias_full.astype(jnp.float32)[None] + masked[:, None, None, :]
    top_score = jnp.max(scores, axis=-1, keepdims=True)
    weights = jnp.exp(scores - top_score)
    attn_probs = weights / jnp.sum(weights, axis=-1, keepdims=True)
    attn_low = attn_probs.astype(jnp.bfloat16)
    attended = jnp.einsum(
        "bhjk,bkhd->bjhd", attn_low, value_heads, preferred_element_type=jnp.float32
    )
    row_delta = jnp.sum(grad_heads.astype(jnp.float32) * attended, axis=-1)
    grad_probs = jnp.einsum(
        "bjhd,bkhd->bhjk", grad_heads, value_heads, preferred_element_type=jnp.float32
    )
    grad_scores = attn_probs * (grad_probs - jnp.transpose(row_delta, (0, 2, 1))[..., None])
    scores_low = grad_scores.astype(jnp.bfloat16)
    grad_queries = (
        jnp.einsum("bhjk,bkhd->bjhd", scores_low, key_heads, preferred_element_type=jnp.float32)
        * scale
    )
    grad_keys = (
        jnp.einsum("bhjk,bjhd->bkhd", scores_low, query_heads, preferred_element_type=jnp.float32)
        * scale
    )
    grad_values = jnp.einsum(
        "bhjk,bjhd->bkhd", attn_low, grad_heads, preferred_element_type=jnp.float32
    )
    bias_grad = jnp.sum(grad_scores, axis=0)
    return (
        grad_queries.reshape(block_rows, query_count, channel_count),
        grad_keys.reshape(block_rows, key_count, channel_count),
        grad_values.reshape(block_rows, key_count, channel_count),
        bias_grad,
    )


def all_blocks(queries, keys_all, values_all, grads, mask_all, bias_full):
    row_count, query_count, channel_count = queries.shape
    key_count = keys_all.shape[1]
    block_rows = 1
    while (
        block_rows * 2 <= row_count
        and row_count % (block_rows * 2) == 0
        and (block_rows * query_count < 512)
    ):
        block_rows = block_rows * 2
    steps_count = row_count // block_rows

    def split_rows(array):
        return array.reshape((steps_count, block_rows) + array.shape[1:])

    def one_block(bias_sum, pieces):
        grad_queries, grad_keys, grad_values, bias_grad = block_grads(
            pieces[0], pieces[1], pieces[2], pieces[3], pieces[4], bias_full
        )
        return (bias_sum + bias_grad, (grad_queries, grad_keys, grad_values))

    start_sum = jnp.zeros((HEADS, query_count, key_count), jnp.float32)
    bias_sum, stacked = lax.scan(
        one_block,
        start_sum,
        (
            split_rows(queries),
            split_rows(keys_all),
            split_rows(values_all),
            split_rows(grads),
            split_rows(mask_all),
        ),
    )
    return (
        stacked[0].reshape(row_count, query_count, channel_count),
        stacked[1].reshape(row_count, key_count, channel_count),
        stacked[2].reshape(row_count, key_count, channel_count),
        bias_sum,
    )


def local(query_proj, key_proj, value_proj, pair_bias, pair_mask, grad_out):
    bias_rows = lax.all_gather(pair_bias, "row", axis=2, tiled=True)
    mask_low = pair_mask.astype(jnp.bfloat16)
    local_tiles = (
        lax.all_to_all(query_proj, "col", split_axis=0, concat_axis=1, tiled=True),
        lax.all_to_all(key_proj, "col", split_axis=0, concat_axis=1, tiled=True),
        lax.all_to_all(value_proj, "col", split_axis=0, concat_axis=1, tiled=True),
        lax.all_to_all(grad_out, "col", split_axis=0, concat_axis=1, tiled=True),
        lax.all_to_all(mask_low, "col", split_axis=0, concat_axis=1, tiled=True),
    )
    bias_full = lax.all_gather(bias_rows, "col", axis=1, tiled=True)
    grad_queries, grad_keys, grad_values, bias_whole = all_blocks(
        local_tiles[0], local_tiles[1], local_tiles[2], local_tiles[3], local_tiles[4], bias_full
    )
    grad_query, grad_key, grad_value = (
        lax.all_to_all(
            grad_queries.astype(jnp.bfloat16), "col", split_axis=1, concat_axis=0, tiled=True
        ),
        lax.all_to_all(
            grad_keys.astype(jnp.bfloat16), "col", split_axis=1, concat_axis=0, tiled=True
        ),
        lax.all_to_all(
            grad_values.astype(jnp.bfloat16), "col", split_axis=1, concat_axis=0, tiled=True
        ),
    )
    bias_part = lax.psum_scatter(bias_whole, "col", scatter_dimension=1, tiled=True)
    grad_bias = lax.psum_scatter(bias_part, "row", scatter_dimension=2, tiled=True)
    return (grad_query, grad_key, grad_value, grad_bias)


MESH = pl.DeviceIdType.MESH


def round_up(value, step):
    return -(-value // step) * step


def fused_kernel(
    rows_n, cols_n, pack,
    q_ref, k_ref, v_ref, g_ref, bias_in, mask_in,
    gq_ref, gk_ref, gv_ref, gb_ref,
    bias_send, got, stage, bias_all, mask_all, bias_full, bias_sum, part, part_in, tile, tile_in,
    in_recv, sems, own_sem,
):
    row, col = lax.axis_index("row"), lax.axis_index("col")
    per = got.shape[1]
    count = got.shape[2]
    width = q_ref.shape[1]
    keys = bias_sum.shape[1] // rows_n
    rows_here = mask_in.shape[0]
    _, packs, padded, lanes = bias_send.shape
    chunk = 2 if per % 2 == 0 else 1
    chunks = per // chunk
    scale = 1.0 / math.sqrt(HEAD_DIM)
    sources = (q_ref, k_ref, v_ref, g_ref)
    results = (gq_ref, gk_ref, gv_ref)
    others = (cols_n - 1) * width
    in_send, out_send, out_recv, bc_send, bc_recv, br_send, br_recv, pr_send, pr_recv, pc_send, pc_recv = (
        sems.at[n] for n in range(11)
    )

    def row_peer(d):
        return (lax.rem(row + d, rows_n), col)

    paired = cols_n & (cols_n - 1) == 0

    def col_peer(d):
        if not paired:
            return (row, lax.rem(col + d, cols_n))
        other = 0
        bit = 1
        while bit < cols_n:
            mine = lax.rem(col // bit, 2)
            other = other + bit * (1 - mine if d & bit else mine)
            bit = bit * 2
        return (row, other)

    def remote(src, dst, send, recv, peer):
        return pltpu.make_async_remote_copy(
            src_ref=src, dst_ref=dst, send_sem=send, recv_sem=recv,
            device_id=peer, device_id_type=MESH,
        )

    nn = (((1,), (0,)), ((), ()))
    nt = (((1,), (1,)), ((), ()))
    tn = (((0,), (0,)), ((), ()))
    barrier = pltpu.get_barrier_semaphore()
    for d in range(1, cols_n):
        pl.semaphore_signal(barrier, inc=1, device_id=col_peer(d), device_id_type=MESH)
    for d in range(1, rows_n):
        pl.semaphore_signal(barrier, inc=1, device_id=row_peer(d), device_id_type=MESH)
    my_cols = pl.ds(pl.multiple_of(col * width, width), width)
    for a in range(4):
        pltpu.make_async_copy(
            sources[a].at[pl.ds(col * per, per)], got.at[a, :, my_cols], own_sem
        ).start()

    def shifted(shape, shift):
        at = lax.broadcasted_iota(jnp.int32, shape, 0)
        lane = lax.broadcasted_iota(jnp.int32, shape, 1)
        return jnp.where(lane == at + shift, 1.0, 0.0).astype(jnp.bfloat16)

    mask_low = mask_in[...].astype(jnp.float32).astype(jnp.bfloat16)
    bases = []
    for p in range(packs):
        flipped = jnp.zeros((keys, lanes), jnp.float32)
        for hh in range(pack):
            flipped = flipped + lax.dot_general(
                bias_in[p * pack + hh], shifted((width, lanes), hh * width), nn,
                preferred_element_type=jnp.float32,
            )
        bases.append(flipped.astype(jnp.bfloat16))
    wide_mask = lax.dot_general(
        mask_low, shifted((width, lanes), 0), nn, preferred_element_type=jnp.float32
    ).astype(jnp.bfloat16)
    for z in range(cols_n):
        for p in range(packs):
            bias_send[z, p, 0:keys, :] = bases[p]
        at = lax.broadcasted_iota(jnp.int32, (padded - keys, rows_here), 0)
        pos = lax.broadcasted_iota(jnp.int32, (padded - keys, rows_here), 1)
        pick_rows = jnp.where((pos == at + z * per) & (at < per), 1.0, 0.0).astype(jnp.bfloat16)
        piece = jnp.dot(pick_rows, wide_mask, preferred_element_type=jnp.float32)
        bias_send[z, 0, keys:padded, :] = piece.astype(jnp.bfloat16)
        for p in range(1, packs):
            bias_send[z, p, keys:padded, :] = jnp.zeros((padded - keys, lanes), jnp.bfloat16)
    bias_all[row, col] = bias_send[col]
    pl.semaphore_wait(barrier, rows_n + cols_n - 2)

    for d in range(1, cols_n):
        peer = col_peer(d)
        remote(bias_send.at[peer[1]], bias_all.at[row, col], bc_send, bc_recv, peer).start()

    @pl.loop(0, chunks)
    def _(c):
        for d in reversed(range(1, cols_n)):
            peer = col_peer(d)
            for a in range(4):
                remote(
                    sources[a].at[pl.ds(peer[1] * per + c * chunk, chunk)],
                    got.at[a, pl.ds(c * chunk, chunk), my_cols],
                    in_send, in_recv.at[c], peer,
                ).start()

    def out_start(c):
        for d in reversed(range(1, cols_n)):
            peer = col_peer(d)
            there = pl.ds(pl.multiple_of(peer[1] * width, width), width)
            for a in range(3):
                remote(
                    stage.at[a, pl.ds(c * chunk, chunk), there],
                    results[a].at[pl.ds(col * per + c * chunk, chunk)],
                    out_send, out_recv, peer,
                ).start()

    bias_sum[...] = jnp.zeros_like(bias_sum)
    part[...] = jnp.zeros_like(part)
    near = col_peer(1)
    side = row_peer(1)
    first = bias_all.at[0, 0:cols_n - 1]
    remote(first, first, bc_send, bc_recv, near).wait_recv()
    for d in range(1, rows_n):
        remote(bias_all.at[row], bias_all.at[row], br_send, br_recv, row_peer(d)).start()
    mask_sum = jnp.zeros((count, padded - keys), jnp.float32)
    for z in range(cols_n):
        at = lax.broadcasted_iota(jnp.int32, (count, lanes), 0)
        lane = lax.broadcasted_iota(jnp.int32, (count, lanes), 1)
        lift = jnp.where((lane < width) & (at == lane + z * width), 1.0, 0.0).astype(jnp.bfloat16)
        mask_sum = mask_sum + lax.dot_general(
            lift, bias_all[row, z, 0, keys:padded, :], nt, preferred_element_type=jnp.float32
        )
    mask_all[...] = mask_sum
    pltpu.make_async_copy(got.at[:, :, my_cols], got.at[:, :, my_cols], own_sem).wait()
    most = bias_all.at[0:rows_n - 1]
    remote(most, most, br_send, br_recv, side).wait_recv()

    def pick(z, hh, shape, lane_axis):
        lane = lax.broadcasted_iota(jnp.int32, shape, lane_axis)
        at = lax.broadcasted_iota(jnp.int32, shape, 1 - lane_axis)
        inside = (lane >= hh * width) & (lane < (hh + 1) * width)
        return jnp.where(inside & (lane + (z - hh) * width == at), 1.0, 0.0).astype(jnp.bfloat16)

    for p in range(packs):
        for hh in range(pack):
            whole = jnp.zeros((rows_n * padded, count), jnp.float32)
            for z in range(cols_n):
                piece = bias_all[:, z, p].reshape(rows_n * padded, lanes)
                whole = whole + jnp.dot(
                    piece, pick(z, hh, (lanes, count), 0), preferred_element_type=jnp.float32
                )
            for r in range(rows_n):
                bias_full[p * pack + hh, r * keys:(r + 1) * keys, :] = (
                    whole[r * padded:r * padded + keys]
                )

    channel = lax.broadcasted_iota(jnp.int32, (count, HEADS * HEAD_DIM), 1)
    mask_lane = lax.broadcasted_iota(jnp.int32, mask_all.shape, 1)

    def one_row(i):
        q, k, v, g = got[0, i], got[1, i], got[2, i], got[3, i]
        present = jnp.sum(
            jnp.where(mask_lane == i, mask_all[...], 0.0), axis=1, keepdims=True,
        )
        masked = 1000000000.0 * (present - 1.0)
        gq = jnp.zeros((count, HEADS * HEAD_DIM), jnp.float32)
        gk = gq
        gv = gq
        for h in range(HEADS):
            mine = (channel >= h * HEAD_DIM) & (channel < (h + 1) * HEAD_DIM)

            def only(x):
                return jnp.where(mine, x, jnp.zeros_like(x))

            kh, vh, qh, gh = only(k), only(v), only(q), only(g)
            scores = lax.dot_general(kh, q, nt, preferred_element_type=jnp.float32) * scale
            scores = scores + bias_full[h] + masked
            weights = jnp.exp(scores - jnp.max(scores, axis=0, keepdims=True))
            probs = weights * (1.0 / jnp.sum(weights, axis=0, keepdims=True))
            low = probs.astype(jnp.bfloat16)
            grad_probs = lax.dot_general(vh, g, nt, preferred_element_type=jnp.float32)
            delta = jnp.sum(low.astype(jnp.float32) * grad_probs, axis=0, keepdims=True)
            grad_scores = probs * (grad_probs - delta)
            bias_sum[h] += grad_scores
            slow = grad_scores.astype(jnp.bfloat16)
            gq = gq + lax.dot_general(slow, kh, tn, preferred_element_type=jnp.float32)
            gk = gk + jnp.dot(slow, qh, preferred_element_type=jnp.float32)
            gv = gv + jnp.dot(low, gh, preferred_element_type=jnp.float32)
        stage[0, i] = (gq * scale).astype(jnp.bfloat16)
        stage[1, i] = (gk * scale).astype(jnp.bfloat16)
        stage[2, i] = gv.astype(jnp.bfloat16)

    @pl.loop(0, chunks)
    def _(c):
        landed = got.at[:, pl.ds(c * chunk, chunk), 0:others]
        remote(landed, landed, in_send, in_recv.at[c], near).wait_recv()

        @pl.loop(0, chunk)
        def _(r):
            one_row(c * chunk + r)

        out_start(c)
        for a in range(3):
            results[a][pl.ds(col * per + c * chunk, chunk)] = (
                stage[a, pl.ds(c * chunk, chunk), my_cols]
            )

    for r in range(rows_n):
        for h in range(HEADS):
            part[r, h, 0:keys, :] = bias_sum[h, r * keys:(r + 1) * keys, :].astype(jnp.bfloat16)
    for d in range(1, rows_n):
        peer = row_peer(d)
        remote(part.at[peer[0]], part_in.at[row], pr_send, pr_recv, peer).start()
    many = part_in.at[0:rows_n - 1]
    remote(many, many, pr_send, pr_recv, side).wait_recv()
    sums = []
    for h in range(HEADS):
        total = part[row, h].astype(jnp.float32)
        for d in range(1, rows_n):
            total = total + part_in[lax.rem(row + d, rows_n), h].astype(jnp.float32)
        sums.append(total.astype(jnp.bfloat16))
    for z in range(cols_n):
        for p in range(packs):
            packed = jnp.zeros((padded, lanes), jnp.float32)
            for hh in range(pack):
                packed = packed + jnp.dot(
                    sums[p * pack + hh], pick(z, hh, (count, lanes), 1),
                    preferred_element_type=jnp.float32,
                )
            tile[z, p] = packed.astype(jnp.bfloat16)
    for d in range(1, cols_n):
        peer = col_peer(d)
        remote(tile.at[peer[1]], tile_in.at[col], pc_send, pc_recv, peer).start()
    few = tile_in.at[0:cols_n - 1]
    remote(few, few, pc_send, pc_recv, near).wait_recv()
    total = tile[col].astype(jnp.float32)
    for d in range(1, cols_n):
        total = total + tile_in[lax.rem(col + d, cols_n)].astype(jnp.float32)
    for p in range(packs):
        for hh in range(pack):
            gb_ref[p * pack + hh] = total[p, 0:keys, hh * width:(hh + 1) * width]

    ins = got.at[:, :, 0:others]
    outs = stage.at[:, :, 0:others]
    for ref, send in (
        (ins, in_send), (outs, out_send), (first, bc_send), (most, br_send),
        (many, pr_send), (few, pc_send),
    ):
        remote(ref, ref, send, send, near).wait_send()
    remote(outs, outs, out_send, out_recv, near).wait_recv()


def writer_kernel(*refs):
    count = len(refs) // 2
    sem = refs[-1]
    copies = [
        pltpu.make_async_copy(refs[n], refs[count + n], sem.at[n]) for n in range(count)
    ]
    for copy in copies:
        copy.start()
    for copy in copies:
        copy.wait()


def written(*arrays):
    return pl.pallas_call(
        writer_kernel,
        name="write_grads",
        out_shape=tuple(jax.ShapeDtypeStruct(a.shape, a.dtype) for a in arrays),
        in_specs=[pl.BlockSpec(memory_space=pl.ANY)] * len(arrays),
        out_specs=(pl.BlockSpec(memory_space=pl.ANY),) * len(arrays),
        scratch_shapes=[pltpu.SemaphoreType.DMA((len(arrays),))],
    )(*(pltpu.with_memory_space_constraint(a, pltpu.VMEM) for a in arrays))


def fused(rows_n, cols_n, query_proj, key_proj, value_proj, pair_bias, pair_mask, grad_out):
    rows, width, channels = query_proj.shape
    keys = pair_bias.shape[2]
    per, count = rows // cols_n, width * cols_n
    pack = 1
    while pack * 2 <= HEADS and pack * 2 * width <= 128:
        pack = pack * 2
    packs = HEADS // pack
    padded, lanes = round_up(keys + per, 16), round_up(pack * width, 128)
    chunk = 2 if per % 2 == 0 else 1
    chunks = per // chunk
    bf16, f32 = jnp.bfloat16, jnp.float32
    anywhere = pl.BlockSpec(memory_space=pl.ANY)
    on_chip = pl.BlockSpec(memory_space=pltpu.VMEM)
    sem = pltpu.SemaphoreType.DMA
    tile_shape = pltpu.VMEM(query_proj.shape, bf16)
    grads = pl.pallas_call(
        functools.partial(fused_kernel, rows_n, cols_n, pack),
        name="triangle_grads",
        out_shape=(
            tile_shape, tile_shape, tile_shape,
            pltpu.VMEM((HEADS, keys, width), f32),
        ),
        in_specs=[anywhere] * 4 + [on_chip] * 2,
        out_specs=(on_chip,) * 4,
        scratch_shapes=[
            pltpu.VMEM((cols_n, packs, padded, lanes), bf16),
            pltpu.VMEM((4, per, count, channels), bf16),
            pltpu.VMEM((3, per, count, channels), bf16),
            pltpu.VMEM((rows_n, cols_n, packs, padded, lanes), bf16),
            pltpu.VMEM((count, padded - keys), f32),
            pltpu.VMEM((HEADS, count, count), f32),
            pltpu.VMEM((HEADS, count, count), f32),
            pltpu.VMEM((rows_n, HEADS, padded, count), bf16),
            pltpu.VMEM((rows_n, HEADS, padded, count), bf16),
            pltpu.VMEM((cols_n, packs, padded, lanes), bf16),
            pltpu.VMEM((cols_n, packs, padded, lanes), bf16),
            sem((chunks,)), sem((11,)), sem(()),
        ],
        compiler_params=pltpu.CompilerParams(collective_id=0, has_side_effects=True),
    )(query_proj, key_proj, value_proj, grad_out, jnp.transpose(pair_bias, (0, 2, 1)), pair_mask)
    gq, gk, gv, gb = written(*grads)
    return gq, gk, gv, jnp.transpose(gb, (0, 2, 1))


def choose(rows_n, cols_n):
    def run(*arrays):
        count = arrays[0].shape[1] * cols_n
        if count * count * 4 <= 512 * 1024 and arrays[0].shape[0] % cols_n == 0:
            return fused(rows_n, cols_n, *arrays)
        return local(*arrays)

    return run


def solution(mesh):
    placed = (
        P("row", "col", None),
        P("row", "col", None),
        P("row", "col", None),
        P(None, "col", "row"),
        P("row", "col"),
        P("row", "col", None),
    )
    return jax.shard_map(
        choose(mesh.shape["row"], mesh.shape["col"]),
        mesh=mesh,
        in_specs=placed,
        out_specs=(
            P("row", "col", None),
            P("row", "col", None),
            P("row", "col", None),
            P(None, "col", "row"),
        ),
        check_vma=False,
    )
```

```python
import functools
import math

import jax
import jax.numpy as jnp
from jax import lax
from jax.experimental import pallas as pl
from jax.experimental.pallas import tpu as pltpu
from jax.sharding import PartitionSpec as P

HEADS = 4
HEAD_DIM = 32


def block_grads(queries, keys_all, values_all, grads, mask_all, bias_full):
    block_rows, query_count, channel_count = queries.shape
    key_count = keys_all.shape[1]
    scale = 1.0 / math.sqrt(HEAD_DIM)
    query_heads = queries.reshape(block_rows, query_count, HEADS, HEAD_DIM)
    key_heads = keys_all.reshape(block_rows, key_count, HEADS, HEAD_DIM)
    value_heads = values_all.reshape(block_rows, key_count, HEADS, HEAD_DIM)
    grad_heads = grads.reshape(block_rows, query_count, HEADS, HEAD_DIM)
    masked = 1000000000.0 * (mask_all.astype(jnp.float32) - 1.0)
    scores = (
        jnp.einsum("bjhd,bkhd->bhjk", query_heads, key_heads, preferred_element_type=jnp.float32)
        * scale
    )
    scores = scores + bias_full.astype(jnp.float32)[None] + masked[:, None, None, :]
    top_score = jnp.max(scores, axis=-1, keepdims=True)
    weights = jnp.exp(scores - top_score)
    attn_probs = weights / jnp.sum(weights, axis=-1, keepdims=True)
    attn_low = attn_probs.astype(jnp.bfloat16)
    attended = jnp.einsum(
        "bhjk,bkhd->bjhd", attn_low, value_heads, preferred_element_type=jnp.float32
    )
    row_delta = jnp.sum(grad_heads.astype(jnp.float32) * attended, axis=-1)
    grad_probs = jnp.einsum(
        "bjhd,bkhd->bhjk", grad_heads, value_heads, preferred_element_type=jnp.float32
    )
    grad_scores = attn_probs * (grad_probs - jnp.transpose(row_delta, (0, 2, 1))[..., None])
    scores_low = grad_scores.astype(jnp.bfloat16)
    grad_queries = (
        jnp.einsum("bhjk,bkhd->bjhd", scores_low, key_heads, preferred_element_type=jnp.float32)
        * scale
    )
    grad_keys = (
        jnp.einsum("bhjk,bjhd->bkhd", scores_low, query_heads, preferred_element_type=jnp.float32)
        * scale
    )
    grad_values = jnp.einsum(
        "bhjk,bjhd->bkhd", attn_low, grad_heads, preferred_element_type=jnp.float32
    )
    bias_grad = jnp.sum(grad_scores, axis=0)
    return (
        grad_queries.reshape(block_rows, query_count, channel_count),
        grad_keys.reshape(block_rows, key_count, channel_count),
        grad_values.reshape(block_rows, key_count, channel_count),
        bias_grad,
    )


def all_blocks(queries, keys_all, values_all, grads, mask_all, bias_full):
    row_count, query_count, channel_count = queries.shape
    key_count = keys_all.shape[1]
    block_rows = 1
    while (
        block_rows * 2 <= row_count
        and row_count % (block_rows * 2) == 0
        and (block_rows * query_count < 512)
    ):
        block_rows = block_rows * 2
    steps_count = row_count // block_rows

    def split_rows(array):
        return array.reshape((steps_count, block_rows) + array.shape[1:])

    def one_block(bias_sum, pieces):
        grad_queries, grad_keys, grad_values, bias_grad = block_grads(
            pieces[0], pieces[1], pieces[2], pieces[3], pieces[4], bias_full
        )
        return (bias_sum + bias_grad, (grad_queries, grad_keys, grad_values))

    start_sum = jnp.zeros((HEADS, query_count, key_count), jnp.float32)
    bias_sum, stacked = lax.scan(
        one_block,
        start_sum,
        (
            split_rows(queries),
            split_rows(keys_all),
            split_rows(values_all),
            split_rows(grads),
            split_rows(mask_all),
        ),
    )
    return (
        stacked[0].reshape(row_count, query_count, channel_count),
        stacked[1].reshape(row_count, key_count, channel_count),
        stacked[2].reshape(row_count, key_count, channel_count),
        bias_sum,
    )


def local(query_proj, key_proj, value_proj, pair_bias, pair_mask, grad_out):
    bias_rows = lax.all_gather(pair_bias, "row", axis=2, tiled=True)
    mask_low = pair_mask.astype(jnp.bfloat16)
    local_tiles = (
        lax.all_to_all(query_proj, "col", split_axis=0, concat_axis=1, tiled=True),
        lax.all_to_all(key_proj, "col", split_axis=0, concat_axis=1, tiled=True),
        lax.all_to_all(value_proj, "col", split_axis=0, concat_axis=1, tiled=True),
        lax.all_to_all(grad_out, "col", split_axis=0, concat_axis=1, tiled=True),
        lax.all_to_all(mask_low, "col", split_axis=0, concat_axis=1, tiled=True),
    )
    bias_full = lax.all_gather(bias_rows, "col", axis=1, tiled=True)
    grad_queries, grad_keys, grad_values, bias_whole = all_blocks(
        local_tiles[0], local_tiles[1], local_tiles[2], local_tiles[3], local_tiles[4], bias_full
    )
    grad_query, grad_key, grad_value = (
        lax.all_to_all(
            grad_queries.astype(jnp.bfloat16), "col", split_axis=1, concat_axis=0, tiled=True
        ),
        lax.all_to_all(
            grad_keys.astype(jnp.bfloat16), "col", split_axis=1, concat_axis=0, tiled=True
        ),
        lax.all_to_all(
            grad_values.astype(jnp.bfloat16), "col", split_axis=1, concat_axis=0, tiled=True
        ),
    )
    bias_part = lax.psum_scatter(bias_whole, "col", scatter_dimension=1, tiled=True)
    grad_bias = lax.psum_scatter(bias_part, "row", scatter_dimension=2, tiled=True)
    return (grad_query, grad_key, grad_value, grad_bias)


MESH = pl.DeviceIdType.MESH


def round_up(value, step):
    return -(-value // step) * step


AHEAD = 3
OWN_AHEAD = 6
LAG = 5
QUERIES_FIRST = 5
OUT_FROM = 4


def split_kernel(
    rows_n, pack,
    q_ref, k_ref, v_ref, g_ref, bias_in, mask_in,
    gq_ref, gk_ref, gv_ref, gb_ref,
    bias_send, bias_got, bias_rows, bias_half, mask_send, mask_half, qg, kv, scores_at, probs_at,
    stats, stats_in, stage_q, stage_kv, stage_sum, gq_in, bias_sum, part, part_in, tile, tile_in,
    from_outer, keys_in, from_mate, stats_recv, gq_recv, own_recv, sems,
):
    row, col = lax.axis_index("row"), lax.axis_index("col")
    cols_n = 4
    rows, width, _ = q_ref.shape
    chunk = rows // from_outer.shape[0]
    chunks = rows // chunk
    half, count = 2 * width, cols_n * width
    upper = rows_n // 2
    keys = half // upper
    packs, padded, lanes = bias_send.shape
    scale = 1.0 / math.sqrt(HEAD_DIM)
    (own_sem, outer_send, mate_send, stats_send, gq_send, kv_send, kv_recv, mask_out, mask_got,
     bz_send, bz_recv, br_send, br_recv, pr_send, pr_recv, pc_send, pc_recv) = (
        sems.at[n] for n in range(17)
    )
    inner = (col == 1) | (col == 2)
    home = 1 + col // 2
    mate = 3 - col
    outer = 3 * (home - 1)
    bias_home = 1 + row // upper
    holder = col == bias_home
    slot = lax.rem(row, upper)
    local = lax.rem(col, 2) * width
    local_outer = width - local

    def at_block(position):
        return pl.ds(pl.multiple_of(position * width, width), width)

    def remote(src, dst, send, recv, peer):
        return pltpu.make_async_remote_copy(
            src_ref=src, dst_ref=dst, send_sem=send, recv_sem=recv,
            device_id=peer, device_id_type=MESH,
        )

    next_col = (row, lax.rem(col + 1, cols_n))

    def landed(ref, sem):
        remote(ref, ref, sem, sem, next_col).wait_recv()

    def left(ref, sem):
        remote(ref, ref, sem, sem, next_col).wait_send()

    nn = (((1,), (0,)), ((), ()))
    nt = (((1,), (1,)), ((), ()))
    tn = (((0,), (0,)), ((), ()))
    barrier = pltpu.get_barrier_semaphore()
    for d in range(1, cols_n):
        pl.semaphore_signal(
            barrier, inc=1, device_id=(row, lax.rem(col + d, cols_n)), device_id_type=MESH
        )
    for d in range(1, rows_n):
        pl.semaphore_signal(
            barrier, inc=1, device_id=(lax.rem(row + d, rows_n), col), device_id_type=MESH
        )
    my_block = at_block(col)
    mate_half = pl.ds(pl.multiple_of((2 - home) * half, half), half)

    @pl.when(inner)
    def _():
        for a, ref in enumerate((q_ref, g_ref)):
            pltpu.make_async_copy(ref, qg.at[a, :, my_block], own_sem).start()
        for a, ref in enumerate((k_ref, v_ref)):
            pltpu.make_async_copy(ref, kv.at[a, :, pl.ds(local, width)], own_sem).start()

    def shifted(shape, shift):
        at = lax.broadcasted_iota(jnp.int32, shape, 0)
        lane = lax.broadcasted_iota(jnp.int32, shape, 1)
        return jnp.where(lane == at + shift, 1.0, 0.0).astype(jnp.bfloat16)

    bias_send[...] = jnp.zeros_like(bias_send)
    for p in range(packs):
        flipped = jnp.zeros((keys, lanes), jnp.float32)
        for hh in range(pack):
            flipped = flipped + lax.dot_general(
                bias_in[p * pack + hh], shifted((width, lanes), hh * width), nn,
                preferred_element_type=jnp.float32,
            )
        bias_send[p, 0:keys, :] = flipped.astype(jnp.bfloat16)
    mask_send[...] = lax.dot_general(
        mask_in[...].astype(jnp.float32).astype(jnp.bfloat16),
        shifted((rows, mask_send.shape[1]), 0), tn, preferred_element_type=jnp.float32,
    ).astype(jnp.bfloat16)
    pl.semaphore_wait(barrier, rows_n + cols_n - 2)

    bias_piece = remote(
        bias_send, bias_got.at[col], bz_send, bz_recv, (row, bias_home)
    )

    @pl.when(jnp.logical_not(holder))
    def _():
        bias_piece.start()

    def rows_of(c):
        return pl.ds(c * chunk, chunk)

    @pl.when(jnp.logical_not(inner))
    def _():
        remote(
            mask_send, mask_half.at[pl.ds(local, width)], mask_out, mask_got, (row, home)
        ).start()

        def queries_start(c):
            for a, ref in enumerate((q_ref, g_ref)):
                remote(
                    ref.at[rows_of(c)], qg.at[a, rows_of(c), my_block],
                    outer_send, from_outer.at[c], (row, home),
                ).start()

        ahead = min(QUERIES_FIRST, chunks)
        pl.loop(0, ahead)(queries_start)

        @pl.loop(0, chunks)
        def _(c):
            for a, ref in enumerate((k_ref, v_ref)):
                remote(
                    ref.at[rows_of(c)], kv.at[a, rows_of(c), pl.ds(local, width)],
                    outer_send, keys_in.at[c], (row, home),
                ).start()

            @pl.when(c + ahead < chunks)
            def _():
                queries_start(c + ahead)

    def pick(z, hh, shape, lane_axis):
        lane = lax.broadcasted_iota(jnp.int32, shape, lane_axis)
        at = lax.broadcasted_iota(jnp.int32, shape, 1 - lane_axis)
        inside = (lane >= hh * width) & (lane < (hh + 1) * width)
        return jnp.where(inside & (lane + (z - hh) * width == at), 1.0, 0.0).astype(jnp.bfloat16)

    channel = lax.broadcasted_iota(jnp.int32, (1, HEADS * HEAD_DIM), 1)

    def only(x, h):
        mine = (channel >= h * HEAD_DIM) & (channel < (h + 1) * HEAD_DIM)
        return jnp.where(mine, x, jnp.zeros_like(x))

    def own_start(c):
        for a, ref in enumerate((q_ref, g_ref)):
            remote(
                ref.at[rows_of(c)], qg.at[a, rows_of(c), my_block],
                mate_send, from_mate.at[c], (row, mate),
            ).start()

    def relay(c):
        block = qg.at[:, rows_of(c), at_block(outer)]
        landed(block, from_outer.at[c])
        for a in range(2):
            block = qg.at[a, rows_of(c), at_block(outer)]
            remote(block, block, mate_send, from_mate.at[c], (row, mate)).start()

        @pl.when(c + OWN_AHEAD < chunks)
        def _():
            own_start(c + OWN_AHEAD)

    def first_pass(c):
        landed(qg.at[:, rows_of(c), mate_half], from_mate.at[c])
        landed(kv.at[:, rows_of(c), pl.ds(local_outer, width)], keys_in.at[c])
        there = lax.rem(c, LAG + 1)
        mask_lane = lax.broadcasted_iota(jnp.int32, mask_half.shape, 1)
        rows_stats = []
        for r in range(chunk):
            i = c * chunk + r
            q, g, k, v = qg[0, i], qg[1, i], kv[0, i], kv[1, i]
            present = jnp.sum(
                jnp.where(mask_lane == i, mask_half[...].astype(jnp.float32), 0.0),
                axis=1, keepdims=True,
            )
            masked = 1000000000.0 * (present - 1.0)
            some = jnp.max(present, axis=0, keepdims=True)
            shift = jnp.where(some > 0.0, 0.0, 1000000000.0 - 4096.0)
            stacked_keys = jnp.concatenate([only(k, h) for h in range(HEADS)], axis=0)
            stacked_values = jnp.concatenate([only(v, h) for h in range(HEADS)], axis=0)
            raw = lax.dot_general(stacked_keys, q, nt, preferred_element_type=jnp.float32)
            grad_probs = lax.dot_general(stacked_values, g, nt, preferred_element_type=jnp.float32)
            logs, deltas = [], []
            for h in range(HEADS):
                part_rows = slice(h * half, (h + 1) * half)
                score = raw[part_rows] * scale + bias_half[h]
                score = (score + masked) + shift
                grad_prob = grad_probs[part_rows]
                top = jnp.max(score, axis=0, keepdims=True)
                weights = jnp.exp(score - top)
                total = jnp.sum(weights, axis=0, keepdims=True)
                logs.append(top + jnp.log(total))
                deltas.append(jnp.sum(weights * grad_prob, axis=0, keepdims=True) / total)
                scores_at[there, r, h] = score
                probs_at[there, r, h] = grad_prob
            rows_stats.append(jnp.concatenate(logs + deltas, axis=0))
        stats[c] = jnp.concatenate(rows_stats, axis=1)
        remote(stats.at[c], stats_in.at[c], stats_send, stats_recv.at[c], (row, mate)).start()

    def second_pass(c):
        landed(stats_in.at[c], stats_recv.at[c])
        there = lax.rem(c, LAG + 1)
        here, other = stats[c], stats_in[c]
        log_here, log_other = here[0:HEADS], other[0:HEADS]
        top = jnp.maximum(log_here, log_other)
        log_all = top + jnp.log(jnp.exp(log_here - top) + jnp.exp(log_other - top))
        delta_all = (
            here[HEADS:2 * HEADS] * jnp.exp(log_here - log_all)
            + other[HEADS:2 * HEADS] * jnp.exp(log_other - log_all)
        )
        gqs = [jnp.zeros((count, HEADS * HEAD_DIM), jnp.float32)] * chunk
        gks = [jnp.zeros((half, HEADS * HEAD_DIM), jnp.float32)] * chunk
        gvs = list(gks)
        for h in range(HEADS):
            bias_part = bias_sum[h]
            for r in range(chunk):
                i = c * chunk + r
                lane_part = slice(r * count, (r + 1) * count)
                probs = jnp.exp(scores_at[there, r, h] - log_all[h:h + 1, lane_part])
                grad_scores = probs * (probs_at[there, r, h] - delta_all[h:h + 1, lane_part])
                bias_part = bias_part + grad_scores
                low, slow = probs.astype(jnp.bfloat16), grad_scores.astype(jnp.bfloat16)
                gqs[r] = gqs[r] + lax.dot_general(
                    slow, only(kv[0, i], h), tn, preferred_element_type=jnp.float32
                )
                gks[r] = gks[r] + jnp.dot(
                    slow, only(qg[0, i], h), preferred_element_type=jnp.float32
                )
                gvs[r] = gvs[r] + jnp.dot(
                    low, only(qg[1, i], h), preferred_element_type=jnp.float32
                )
            bias_sum[h] = bias_part
        for r in range(chunk):
            i = c * chunk + r
            stage_q[i] = (gqs[r] * scale).astype(jnp.bfloat16)
            stage_kv[0, i] = (gks[r] * scale).astype(jnp.bfloat16)
            stage_kv[1, i] = gvs[r].astype(jnp.bfloat16)
        for a, ref in enumerate((gk_ref, gv_ref)):
            remote(
                stage_kv.at[a, rows_of(c), pl.ds(local_outer, width)], ref.at[rows_of(c)],
                kv_send, kv_recv, (row, outer),
            ).start()
            ref[rows_of(c)] = stage_kv[a, rows_of(c), pl.ds(local, width)]

    groups = own_recv.shape[0]
    grouped = chunks // groups

    def outer_part(c):
        remote(
            stage_q.at[rows_of(c), at_block(3 - outer)], gq_in.at[rows_of(c), pl.ds(local, width)],
            gq_send, gq_recv.at[c], (row, mate),
        ).start()

    def own_rows(n):
        return pl.ds(n * grouped * chunk, grouped * chunk)

    def own_part(n):
        remote(
            stage_q.at[own_rows(n), at_block(mate)],
            gq_in.at[own_rows(n), pl.ds(local_outer, width)],
            gq_send, own_recv.at[n], (row, mate),
        ).start()

    def outer_sum(c):
        landed(gq_in.at[rows_of(c), pl.ds(local_outer, width)], gq_recv.at[c])
        total = stage_q[rows_of(c), at_block(outer)].astype(jnp.float32)
        total = total + gq_in[rows_of(c), pl.ds(local_outer, width)].astype(jnp.float32)
        stage_sum[rows_of(c)] = total.astype(jnp.bfloat16)
        remote(
            stage_sum.at[rows_of(c)], gq_ref.at[rows_of(c)], kv_send, kv_recv, (row, outer)
        ).start()

    @pl.when(inner)
    def _():
        for c in range(min(OWN_AHEAD, chunks)):
            own_start(c)
        bias_sum[...] = jnp.zeros_like(bias_sum)
        part[...] = jnp.zeros_like(part)
        mask_half[pl.ds(local, width)] = mask_send[...]

        @pl.when(holder)
        def _():
            bias_got[col] = bias_send[...]
            landed(bias_got.at[0:cols_n - 1], bz_recv)
            for p in range(packs):
                for hh in range(pack):
                    whole = jnp.zeros((padded, count), jnp.float32)
                    for z in range(cols_n):
                        whole = whole + jnp.dot(
                            bias_got[z, p], pick(z, hh, (lanes, count), 0),
                            preferred_element_type=jnp.float32,
                        )
                    bias_rows[slot, p * pack + hh] = whole.astype(jnp.bfloat16)
            for d in range(1, rows_n):
                remote(
                    bias_rows.at[slot], bias_rows.at[slot], br_send, br_recv,
                    (lax.rem(row + d, rows_n), col),
                ).start()

        pltpu.make_async_copy(
            qg.at[:, :, 0:half], qg.at[:, :, 0:half], own_sem
        ).wait()
        landed(mask_half.at[pl.ds(local_outer, width)], mask_got)

        @pl.loop(0, min(AHEAD, chunks))
        def _(c):
            relay(c)

        @pl.when(holder)
        def _():
            landed(bias_rows.at[0:upper - 1], br_recv)

        @pl.when(jnp.logical_not(holder))
        def _():
            landed(bias_rows, br_recv)

        for r in range(upper):
            for h in range(HEADS):
                bias_half[h, r * keys:(r + 1) * keys, :] = (
                    bias_rows[r, h].astype(jnp.float32)[0:keys]
                )

        out_from = max(chunks - OUT_FROM, LAG)
        own_steps = [
            max(out_from + 1 + 2 * n, (n + 1) * grouped - 1 + LAG) for n in range(groups)
        ]

        @pl.loop(0, chunks + LAG)
        def _(c):
            @pl.when(c + AHEAD < chunks)
            def _():
                relay(c + AHEAD)

            @pl.when(c < chunks)
            def _():
                first_pass(c)

            @pl.when(c >= LAG)
            def _():
                second_pass(c - LAG)

            @pl.when(c == out_from)
            def _():
                pl.loop(0, out_from - LAG)(outer_part)

            @pl.when(c >= out_from)
            def _():
                outer_part(c - LAG)

            for n in range(groups - 1):
                pl.when(c == own_steps[n])(functools.partial(own_part, n))

        own_part(groups - 1)

        for r in range(upper):
            for h in range(HEADS):
                part[r, h, 0:keys, :] = bias_sum[h, r * keys:(r + 1) * keys, :].astype(jnp.bfloat16)
        for r in range(upper):
            owner = (col - 1) * upper + r

            @pl.when(owner != row)
            def _():
                remote(part.at[r], part_in.at[row], pr_send, pr_recv, (owner, col)).start()

        pl.loop(0, chunks)(outer_sum)

        @pl.when(holder)
        def _():
            many = part_in.at[0:rows_n - 1]
            landed(many, pr_recv)
            sums = []
            for h in range(HEADS):
                total = part[slot, h].astype(jnp.float32)
                for d in range(1, rows_n):
                    total = total + part_in[lax.rem(row + d, rows_n), h].astype(jnp.float32)
                sums.append(total.astype(jnp.bfloat16))
            for z in range(cols_n):
                for p in range(packs):
                    packed = jnp.zeros((padded, lanes), jnp.float32)
                    for hh in range(pack):
                        packed = packed + jnp.dot(
                            sums[p * pack + hh], pick(z, hh, (count, lanes), 1),
                            preferred_element_type=jnp.float32,
                        )
                    tile[z, p] = packed.astype(jnp.bfloat16)
            for d in range(1, cols_n):
                there = lax.rem(col + d, cols_n)
                remote(tile.at[there], tile_in, pc_send, pc_recv, (row, there)).start()
            tile_in[...] = tile[col]
            left(many, br_send)
            left(part.at[0:upper - 1], pr_send)
            left(tile.at[0:cols_n - 1], pc_send)

        @pl.when(jnp.logical_not(holder))
        def _():
            left(part, pr_send)

        for n in range(groups):
            landed(gq_in.at[own_rows(n), pl.ds(local, width)], own_recv.at[n])

            @pl.loop(n * grouped, (n + 1) * grouped)
            def _(c):
                total = stage_q[rows_of(c), my_block].astype(jnp.float32)
                total = total + gq_in[rows_of(c), pl.ds(local, width)].astype(jnp.float32)
                gq_ref[rows_of(c)] = total.astype(jnp.bfloat16)

        left(qg.at[:, :, 0:half], mate_send)
        left(stats, stats_send)
        left(gq_in, gq_send)
        left(qg.at[0, :, 0:3 * width], kv_send)

    @pl.when(jnp.logical_not(inner))
    def _():
        landed(qg.at[0, :, 0:3 * width], kv_recv)
        left(mask_send, mask_out)
        left(qg.at[:, :, 0:half], outer_send)

    @pl.when(jnp.logical_not(holder))
    def _():
        landed(tile_in, pc_recv)
        bias_piece.wait_send()

    for p in range(packs):
        for hh in range(pack):
            gb_ref[p * pack + hh] = tile_in[
                p, 0:keys, hh * width:(hh + 1) * width
            ].astype(jnp.float32)


def writer_kernel(*refs):
    count = len(refs) // 2
    sem = refs[-1]
    copies = [
        pltpu.make_async_copy(refs[n], refs[count + n], sem.at[n]) for n in range(count)
    ]
    for copy in copies:
        copy.start()
    for copy in copies:
        copy.wait()


def written(*arrays):
    return pl.pallas_call(
        writer_kernel,
        name="write_grads",
        out_shape=tuple(jax.ShapeDtypeStruct(a.shape, a.dtype) for a in arrays),
        in_specs=[pl.BlockSpec(memory_space=pl.ANY)] * len(arrays),
        out_specs=(pl.BlockSpec(memory_space=pl.ANY),) * len(arrays),
        scratch_shapes=[pltpu.SemaphoreType.DMA((len(arrays),))],
    )(*(pltpu.with_memory_space_constraint(a, pltpu.VMEM) for a in arrays))


def fused(rows_n, query_proj, key_proj, value_proj, pair_bias, pair_mask, grad_out):
    rows, width, channels = query_proj.shape
    keys = pair_bias.shape[2]
    cols_n = 4
    half, count, upper = 2 * width, 4 * width, rows_n // 2
    pack = 1
    while pack * 2 <= HEADS and pack * 2 * width <= 128:
        pack = pack * 2
    packs = HEADS // pack
    padded, lanes = round_up(keys, 16), round_up(pack * width, 128)
    mask_lanes = round_up(rows, 128)
    chunk = 2 if rows % 2 == 0 else 1
    chunks = rows // chunk
    bf16, f32 = jnp.bfloat16, jnp.float32
    anywhere = pl.BlockSpec(memory_space=pl.ANY)
    on_chip = pl.BlockSpec(memory_space=pltpu.VMEM)
    sem = pltpu.SemaphoreType.DMA
    tile_shape = pltpu.VMEM(query_proj.shape, bf16)
    grads = pl.pallas_call(
        functools.partial(split_kernel, rows_n, pack),
        name="triangle_grads",
        out_shape=(
            tile_shape, tile_shape, tile_shape,
            pltpu.VMEM((HEADS, keys, width), f32),
        ),
        in_specs=[anywhere] * 4 + [on_chip] * 2,
        out_specs=(on_chip,) * 4,
        scratch_shapes=[
            pltpu.VMEM((packs, padded, lanes), bf16),
            pltpu.VMEM((cols_n, packs, padded, lanes), bf16),
            pltpu.VMEM((upper, HEADS, padded, count), bf16),
            pltpu.VMEM((HEADS, half, count), f32),
            pltpu.VMEM((width, mask_lanes), bf16),
            pltpu.VMEM((half, mask_lanes), bf16),
            pltpu.VMEM((2, rows, count, channels), bf16),
            pltpu.VMEM((2, rows, half, channels), bf16),
            pltpu.VMEM((LAG + 1, chunk, HEADS, half, count), f32),
            pltpu.VMEM((LAG + 1, chunk, HEADS, half, count), f32),
            pltpu.VMEM((chunks, 2 * HEADS, chunk * count), f32),
            pltpu.VMEM((chunks, 2 * HEADS, chunk * count), f32),
            pltpu.VMEM((rows, count, channels), bf16),
            pltpu.VMEM((2, rows, half, channels), bf16),
            pltpu.VMEM((rows, width, channels), bf16),
            pltpu.VMEM((rows, half, channels), bf16),
            pltpu.VMEM((HEADS, half, count), f32),
            pltpu.VMEM((upper, HEADS, padded, count), bf16),
            pltpu.VMEM((rows_n, HEADS, padded, count), bf16),
            pltpu.VMEM((cols_n, packs, padded, lanes), bf16),
            pltpu.VMEM((packs, padded, lanes), bf16),
            sem((chunks,)), sem((chunks,)), sem((chunks,)), sem((chunks,)), sem((chunks,)),
            sem((3 if chunks % 3 == 0 else 1,)), sem((17,)),
        ],
        compiler_params=pltpu.CompilerParams(collective_id=0, has_side_effects=True),
    )(query_proj, key_proj, value_proj, grad_out, jnp.transpose(pair_bias, (0, 2, 1)), pair_mask)
    gq, gk, gv, gb = written(*grads)
    return gq, gk, gv, jnp.transpose(gb, (0, 2, 1))


def choose(rows_n, cols_n):
    def run(*arrays):
        count = arrays[0].shape[1] * cols_n
        small = count * count * 4 <= 512 * 1024 and arrays[0].shape[0] <= 128
        if small and cols_n == 4 and rows_n % 2 == 0 and arrays[0].shape[1] % 16 == 0:
            return fused(rows_n, *arrays)
        return local(*arrays)

    return run


def solution(mesh):
    placed = (
        P("row", "col", None),
        P("row", "col", None),
        P("row", "col", None),
        P(None, "col", "row"),
        P("row", "col"),
        P("row", "col", None),
    )
    return jax.shard_map(
        choose(mesh.shape["row"], mesh.shape["col"]),
        mesh=mesh,
        in_specs=placed,
        out_specs=(
            P("row", "col", None),
            P("row", "col", None),
            P("row", "col", None),
            P(None, "col", "row"),
        ),
        check_vma=False,
    )
```

```python
import functools
import math

import jax
import jax.numpy as jnp
from jax import lax
from jax.experimental import pallas as pl
from jax.experimental.pallas import tpu as pltpu
from jax.sharding import PartitionSpec as P

HEADS = 4
HEAD_DIM = 32


def block_grads(queries, keys_all, values_all, grads, mask_all, bias_full):
    block_rows, query_count, channel_count = queries.shape
    key_count = keys_all.shape[1]
    scale = 1.0 / math.sqrt(HEAD_DIM)
    query_heads = queries.reshape(block_rows, query_count, HEADS, HEAD_DIM)
    key_heads = keys_all.reshape(block_rows, key_count, HEADS, HEAD_DIM)
    value_heads = values_all.reshape(block_rows, key_count, HEADS, HEAD_DIM)
    grad_heads = grads.reshape(block_rows, query_count, HEADS, HEAD_DIM)
    masked = 1000000000.0 * (mask_all.astype(jnp.float32) - 1.0)
    scores = (
        jnp.einsum("bjhd,bkhd->bhjk", query_heads, key_heads, preferred_element_type=jnp.float32)
        * scale
    )
    scores = scores + bias_full.astype(jnp.float32)[None] + masked[:, None, None, :]
    top_score = jnp.max(scores, axis=-1, keepdims=True)
    weights = jnp.exp(scores - top_score)
    attn_probs = weights / jnp.sum(weights, axis=-1, keepdims=True)
    attn_low = attn_probs.astype(jnp.bfloat16)
    attended = jnp.einsum(
        "bhjk,bkhd->bjhd", attn_low, value_heads, preferred_element_type=jnp.float32
    )
    row_delta = jnp.sum(grad_heads.astype(jnp.float32) * attended, axis=-1)
    grad_probs = jnp.einsum(
        "bjhd,bkhd->bhjk", grad_heads, value_heads, preferred_element_type=jnp.float32
    )
    grad_scores = attn_probs * (grad_probs - jnp.transpose(row_delta, (0, 2, 1))[..., None])
    scores_low = grad_scores.astype(jnp.bfloat16)
    grad_queries = (
        jnp.einsum("bhjk,bkhd->bjhd", scores_low, key_heads, preferred_element_type=jnp.float32)
        * scale
    )
    grad_keys = (
        jnp.einsum("bhjk,bjhd->bkhd", scores_low, query_heads, preferred_element_type=jnp.float32)
        * scale
    )
    grad_values = jnp.einsum(
        "bhjk,bjhd->bkhd", attn_low, grad_heads, preferred_element_type=jnp.float32
    )
    bias_grad = jnp.sum(grad_scores, axis=0)
    return (
        grad_queries.reshape(block_rows, query_count, channel_count),
        grad_keys.reshape(block_rows, key_count, channel_count),
        grad_values.reshape(block_rows, key_count, channel_count),
        bias_grad,
    )


def all_blocks(queries, keys_all, values_all, grads, mask_all, bias_full):
    row_count, query_count, channel_count = queries.shape
    key_count = keys_all.shape[1]
    block_rows = 1
    while (
        block_rows * 2 <= row_count
        and row_count % (block_rows * 2) == 0
        and (block_rows * query_count < 512)
    ):
        block_rows = block_rows * 2
    steps_count = row_count // block_rows

    def split_rows(array):
        return array.reshape((steps_count, block_rows) + array.shape[1:])

    def one_block(bias_sum, pieces):
        grad_queries, grad_keys, grad_values, bias_grad = block_grads(
            pieces[0], pieces[1], pieces[2], pieces[3], pieces[4], bias_full
        )
        return (bias_sum + bias_grad, (grad_queries, grad_keys, grad_values))

    start_sum = jnp.zeros((HEADS, query_count, key_count), jnp.float32)
    bias_sum, stacked = lax.scan(
        one_block,
        start_sum,
        (
            split_rows(queries),
            split_rows(keys_all),
            split_rows(values_all),
            split_rows(grads),
            split_rows(mask_all),
        ),
    )
    return (
        stacked[0].reshape(row_count, query_count, channel_count),
        stacked[1].reshape(row_count, key_count, channel_count),
        stacked[2].reshape(row_count, key_count, channel_count),
        bias_sum,
    )


def local(query_proj, key_proj, value_proj, pair_bias, pair_mask, grad_out):
    bias_rows = lax.all_gather(pair_bias, "row", axis=2, tiled=True)
    mask_low = pair_mask.astype(jnp.bfloat16)
    local_tiles = (
        lax.all_to_all(query_proj, "col", split_axis=0, concat_axis=1, tiled=True),
        lax.all_to_all(key_proj, "col", split_axis=0, concat_axis=1, tiled=True),
        lax.all_to_all(value_proj, "col", split_axis=0, concat_axis=1, tiled=True),
        lax.all_to_all(grad_out, "col", split_axis=0, concat_axis=1, tiled=True),
        lax.all_to_all(mask_low, "col", split_axis=0, concat_axis=1, tiled=True),
    )
    bias_full = lax.all_gather(bias_rows, "col", axis=1, tiled=True)
    grad_queries, grad_keys, grad_values, bias_whole = all_blocks(
        local_tiles[0], local_tiles[1], local_tiles[2], local_tiles[3], local_tiles[4], bias_full
    )
    grad_query, grad_key, grad_value = (
        lax.all_to_all(
            grad_queries.astype(jnp.bfloat16), "col", split_axis=1, concat_axis=0, tiled=True
        ),
        lax.all_to_all(
            grad_keys.astype(jnp.bfloat16), "col", split_axis=1, concat_axis=0, tiled=True
        ),
        lax.all_to_all(
            grad_values.astype(jnp.bfloat16), "col", split_axis=1, concat_axis=0, tiled=True
        ),
    )
    bias_part = lax.psum_scatter(bias_whole, "col", scatter_dimension=1, tiled=True)
    grad_bias = lax.psum_scatter(bias_part, "row", scatter_dimension=2, tiled=True)
    return (grad_query, grad_key, grad_value, grad_bias)


MESH = pl.DeviceIdType.MESH


def round_up(value, step):
    return -(-value // step) * step


AHEAD = 4
OWN_AHEAD = 5
LAG = 4
LAST_SUMS = 1
QUERIES_FIRST = 5
FIRST_OUT = 5
OUT_STEP = 4
SUM_AFTER = 4


def split_kernel(
    rows_n, pack,
    q_ref, k_ref, v_ref, g_ref, bias_in, mask_in,
    gq_ref, gk_ref, gv_ref, gb_ref,
    bias_send, bias_got, bias_rows, bias_half, mask_send, mask_half, qg, kv, scores_at, probs_at,
    logs_here, logs_other, deltas_here, deltas_other, both_stats, stage_q, stage_kv, stage_sum, gq_in, bias_sum, part, part_in, part_long, tile, tile_in,
    from_outer, keys_in, from_mate, stats_recv, gq_recv, own_recv, sems, pc_recv, greets,
):
    row, col = lax.axis_index("row"), lax.axis_index("col")
    cols_n = 4
    rows, width, _ = q_ref.shape
    chunk = rows // from_outer.shape[0]
    chunks = rows // chunk
    half, count = 2 * width, cols_n * width
    upper = rows_n // 2
    keys = half // upper
    packs, padded, lanes = bias_send.shape
    scale = 1.0 / math.sqrt(HEAD_DIM)
    (own_sem, outer_send, mate_send, stats_send, gq_send, kv_send, kv_recv, mask_out, mask_got,
     bz_send, bz_recv, br_send, br_recv, pr_send, pr_recv, pc_send) = (
        sems.at[n] for n in range(16)
    )
    inner = (col == 1) | (col == 2)
    home = 1 + col // 2
    mate = 3 - col
    outer = 3 * (home - 1)
    bias_home = 1 + row // upper
    holder = col == bias_home
    slot = lax.rem(row, upper)
    group = row // upper
    owner = (col - 1) * upper + slot
    bias_long = part_long.at[0:rows_n - 1]
    local = lax.rem(col, 2) * width
    local_outer = width - local

    def at_block(position):
        return pl.ds(pl.multiple_of(position * width, width), width)

    def remote(src, dst, send, recv, peer):
        return pltpu.make_async_remote_copy(
            src_ref=src, dst_ref=dst, send_sem=send, recv_sem=recv,
            device_id=peer, device_id_type=MESH,
        )

    next_col = (row, lax.rem(col + 1, cols_n))

    def landed(ref, sem):
        remote(ref, ref, sem, sem, next_col).wait_recv()

    def left(ref, sem):
        remote(ref, ref, sem, sem, next_col).wait_send()

    nn = (((1,), (0,)), ((), ()))
    nt = (((1,), (1,)), ((), ()))
    tn = (((0,), (0,)), ((), ()))
    barrier = pltpu.get_barrier_semaphore()

    def greet(sem, peer):
        pl.semaphore_signal(sem, inc=1, device_id=peer, device_id_type=MESH)

    beside = []
    bit = 1
    while bit < rows_n:
        beside.append(row + bit - 2 * bit * lax.rem(row // bit, 2))
        bit = bit * 2

    @pl.when(inner)
    def _():
        greet(barrier, (row, mate))
        for other in beside:
            greet(barrier, (other, col))
        greet(barrier, (row, outer))

    my_block = at_block(col)
    mate_half = pl.ds(pl.multiple_of((2 - home) * half, half), half)
    for a, ref in enumerate((q_ref, g_ref)):
        pltpu.make_async_copy(ref, qg.at[a, :, my_block], own_sem).start()
    for a, ref in enumerate((k_ref, v_ref)):
        pltpu.make_async_copy(ref, kv.at[a, :, pl.ds(local, width)], own_sem).start()

    def own_landed():
        pltpu.make_async_copy(qg.at[:, :, 0:half], qg.at[:, :, 0:half], own_sem).wait()

    def shifted(shape, shift):
        at = lax.broadcasted_iota(jnp.int32, shape, 0)
        lane = lax.broadcasted_iota(jnp.int32, shape, 1)
        return jnp.where(lane == at + shift, 1.0, 0.0).astype(jnp.bfloat16)

    def prepare():
        bias_send[...] = jnp.zeros_like(bias_send)
        for p in range(packs):
            flipped = jnp.zeros((keys, lanes), jnp.float32)
            for hh in range(pack):
                flipped = flipped + lax.dot_general(
                    bias_in[p * pack + hh], shifted((width, lanes), hh * width), nn,
                    preferred_element_type=jnp.float32,
                )
            bias_send[p, 0:keys, :] = flipped.astype(jnp.bfloat16)
        mask_send[...] = lax.dot_general(
            mask_in[...].astype(jnp.float32).astype(jnp.bfloat16),
            shifted((rows, mask_send.shape[1]), 0), tn, preferred_element_type=jnp.float32,
        ).astype(jnp.bfloat16)

    bias_piece = remote(
        bias_send, bias_got.at[col], bz_send, bz_recv, (row, bias_home)
    )

    def rows_of(c):
        return pl.ds(c * chunk, chunk)

    def queries_start(c):
        for a in range(2):
            block = qg.at[a, rows_of(c), my_block]
            remote(block, block, outer_send, from_outer.at[c], (row, home)).start()

    def keys_start(c):
        for a in range(2):
            block = kv.at[a, rows_of(c), pl.ds(local, width)]
            remote(block, block, outer_send, keys_in.at[c], (row, home)).start()

    @pl.when(jnp.logical_not(inner))
    def _():
        own_landed()
        pl.semaphore_wait(barrier, 1)
        ahead = min(QUERIES_FIRST, chunks)
        pl.loop(0, min(2, ahead))(queries_start)
        greet(greets.at[0], (row, home))
        prepare()
        remote(
            mask_send, mask_half.at[pl.ds(local, width)], mask_out, mask_got, (row, home)
        ).start()
        pl.semaphore_wait(barrier, 1)
        bias_piece.start()
        pl.loop(min(2, ahead), ahead)(queries_start)

        @pl.loop(0, chunks)
        def _(c):
            keys_start(c)

            @pl.when(c + ahead < chunks)
            def _():
                queries_start(c + ahead)

    def pick(z, hh, shape, lane_axis):
        lane = lax.broadcasted_iota(jnp.int32, shape, lane_axis)
        at = lax.broadcasted_iota(jnp.int32, shape, 1 - lane_axis)
        inside = (lane >= hh * width) & (lane < (hh + 1) * width)
        return jnp.where(inside & (lane + (z - hh) * width == at), 1.0, 0.0).astype(jnp.bfloat16)

    channel = lax.broadcasted_iota(jnp.int32, (1, HEADS * HEAD_DIM), 1)

    def only(x, h):
        mine = (channel >= h * HEAD_DIM) & (channel < (h + 1) * HEAD_DIM)
        return jnp.where(mine, x, jnp.zeros_like(x))

    def own_start(c):
        for a in range(2):
            block = qg.at[a, rows_of(c), my_block]
            remote(block, block, mate_send, from_mate.at[c], (row, mate)).start()

    def relay(c):
        block = qg.at[:, rows_of(c), at_block(outer)]
        landed(block, from_outer.at[c])
        for a in range(2):
            block = qg.at[a, rows_of(c), at_block(outer)]
            remote(block, block, mate_send, from_mate.at[c], (row, mate)).start()

        @pl.when(c + OWN_AHEAD < chunks)
        def _():
            own_start(c + OWN_AHEAD)

    def first_pass(c):
        landed(qg.at[:, rows_of(c), mate_half], from_mate.at[c])
        landed(kv.at[:, rows_of(c), pl.ds(local_outer, width)], keys_in.at[c])
        there = lax.rem(c, LAG + 1)
        mask_lane = lax.broadcasted_iota(jnp.int32, mask_half.shape, 1)
        rows_logs, rows_deltas = [], []
        for r in range(chunk):
            i = c * chunk + r
            q, g, k, v = qg[0, i], qg[1, i], kv[0, i], kv[1, i]
            present = jnp.sum(
                jnp.where(mask_lane == i, mask_half[...].astype(jnp.float32), 0.0),
                axis=1, keepdims=True,
            )
            masked = 1000000000.0 * (present - 1.0)
            some = jnp.max(present, axis=0, keepdims=True)
            shift = jnp.where(some > 0.0, 0.0, 1000000000.0 - 4096.0)
            stacked_keys = jnp.concatenate([only(k, h) for h in range(HEADS)], axis=0)
            stacked_values = jnp.concatenate([only(v, h) for h in range(HEADS)], axis=0)
            raw = lax.dot_general(stacked_keys, q, nt, preferred_element_type=jnp.float32)
            grad_probs = lax.dot_general(stacked_values, g, nt, preferred_element_type=jnp.float32)
            logs, deltas = [], []
            for h in range(HEADS):
                part_rows = slice(h * half, (h + 1) * half)
                score = raw[part_rows] * scale + bias_half[h]
                score = (score + masked) + shift
                grad_prob = grad_probs[part_rows]
                top = jnp.max(score, axis=0, keepdims=True)
                weights = jnp.exp(score - top)
                total = jnp.sum(weights, axis=0, keepdims=True)
                logs.append(top + jnp.log(total))
                deltas.append(jnp.sum(weights * grad_prob, axis=0, keepdims=True) / total)
                scores_at[there, r, h] = score
                probs_at[there, r, h] = grad_prob
            rows_logs.append(jnp.concatenate(logs, axis=0))
            rows_deltas.append(jnp.concatenate(deltas, axis=0))
        logs_here[c] = jnp.concatenate(rows_logs, axis=1)
        deltas_here[c] = jnp.concatenate(rows_deltas, axis=1).astype(jnp.bfloat16)
        for mine, theirs in ((logs_here, logs_other), (deltas_here, deltas_other)):
            remote(mine.at[c], theirs.at[c], stats_send, stats_recv.at[c], (row, mate)).start()

    def second_pass(c):
        landed(both_stats.at[0], stats_recv.at[c])
        there = lax.rem(c, LAG + 1)
        log_here, log_other = logs_here[c], logs_other[c]
        top = jnp.maximum(log_here, log_other)
        log_all = top + jnp.log(jnp.exp(log_here - top) + jnp.exp(log_other - top))
        delta_all = (
            deltas_here[c].astype(jnp.float32) * jnp.exp(log_here - log_all)
            + deltas_other[c].astype(jnp.float32) * jnp.exp(log_other - log_all)
        )
        gqs = [jnp.zeros((count, HEADS * HEAD_DIM), jnp.float32)] * chunk
        gks = [jnp.zeros((half, HEADS * HEAD_DIM), jnp.float32)] * chunk
        gvs = list(gks)
        for h in range(HEADS):
            bias_part = bias_sum[h]
            for r in range(chunk):
                i = c * chunk + r
                lane_part = slice(r * count, (r + 1) * count)
                probs = jnp.exp(scores_at[there, r, h] - log_all[h:h + 1, lane_part])
                grad_scores = probs * (probs_at[there, r, h] - delta_all[h:h + 1, lane_part])
                bias_part = bias_part + grad_scores
                low, slow = probs.astype(jnp.bfloat16), grad_scores.astype(jnp.bfloat16)
                gqs[r] = gqs[r] + lax.dot_general(
                    slow, only(kv[0, i], h), tn, preferred_element_type=jnp.float32
                )
                gks[r] = gks[r] + jnp.dot(
                    slow, only(qg[0, i], h), preferred_element_type=jnp.float32
                )
                gvs[r] = gvs[r] + jnp.dot(
                    low, only(qg[1, i], h), preferred_element_type=jnp.float32
                )
            bias_sum[h] = bias_part
        for r in range(chunk):
            i = c * chunk + r
            stage_q[i] = (gqs[r] * scale).astype(jnp.bfloat16)
            stage_kv[0, i] = (gks[r] * scale).astype(jnp.bfloat16)
            stage_kv[1, i] = gvs[r].astype(jnp.bfloat16)
        for a, ref in enumerate((gk_ref, gv_ref)):
            remote(
                stage_kv.at[a, rows_of(c), pl.ds(local_outer, width)], ref.at[rows_of(c)],
                kv_send, kv_recv, (row, outer),
            ).start()
            ref[rows_of(c)] = stage_kv[a, rows_of(c), pl.ds(local, width)]

    groups = own_recv.shape[0]
    grouped = chunks // groups

    def outer_part(c):
        remote(
            stage_q.at[rows_of(c), at_block(3 - outer)], gq_in.at[rows_of(c), pl.ds(local, width)],
            gq_send, gq_recv.at[c], (row, mate),
        ).start()

    def own_rows(n):
        return pl.ds(n * grouped * chunk, grouped * chunk)

    def own_part(n):
        remote(
            stage_q.at[own_rows(n), at_block(mate)],
            gq_in.at[own_rows(n), pl.ds(local_outer, width)],
            gq_send, own_recv.at[n], (row, mate),
        ).start()

    def outer_sum(c):
        landed(gq_in.at[rows_of(c), pl.ds(local_outer, width)], gq_recv.at[c])
        total = stage_q[rows_of(c), at_block(outer)].astype(jnp.float32)
        total = total + gq_in[rows_of(c), pl.ds(local_outer, width)].astype(jnp.float32)
        stage_sum[rows_of(c)] = total.astype(jnp.bfloat16)
        remote(
            stage_sum.at[rows_of(c)], gq_ref.at[rows_of(c)], kv_send, kv_recv, (row, outer)
        ).start()

    @pl.when(inner)
    def _():
        own_landed()
        pl.semaphore_wait(barrier, 1 + len(beside))
        greet(barrier, (row, outer))

        own_first = min(OWN_AHEAD, chunks)
        pl.loop(0, min(2, own_first))(own_start)
        prepare()

        @pl.when(jnp.logical_not(holder))
        def _():
            bias_piece.start()

        pl.loop(min(2, own_first), own_first)(own_start)
        for n in range(3, greets.shape[0]):
            for other in beside:
                greet(greets.at[n], (other, col))
            pl.semaphore_wait(greets.at[n], len(beside))
        bias_sum[...] = jnp.zeros_like(bias_sum)
        part[...] = jnp.zeros_like(part)
        mask_half[pl.ds(local, width)] = mask_send[...]

        @pl.when(holder)
        def _():
            bias_got[col] = bias_send[...]
            landed(bias_got.at[0:cols_n - 1], bz_recv)
            for p in range(packs):
                for hh in range(pack):
                    whole = jnp.zeros((padded, count), jnp.float32)
                    for z in range(cols_n):
                        whole = whole + jnp.dot(
                            bias_got[z, p], pick(z, hh, (lanes, count), 0),
                            preferred_element_type=jnp.float32,
                        )
                    bias_rows[slot, p * pack + hh] = whole.astype(jnp.bfloat16)
            for d in range(1, rows_n):
                remote(
                    bias_rows.at[slot], bias_rows.at[slot], br_send, br_recv,
                    (lax.rem(row + d, rows_n), col),
                ).start()

        pl.semaphore_wait(greets.at[0], 1)
        greet(greets.at[1], (row, mate))
        landed(mask_half.at[pl.ds(local_outer, width)], mask_got)

        @pl.loop(0, min(AHEAD, chunks))
        def _(c):
            relay(c)

        @pl.when(holder)
        def _():
            landed(bias_rows.at[0:upper - 1], br_recv)

        @pl.when(jnp.logical_not(holder))
        def _():
            landed(bias_rows, br_recv)

        for r in range(upper):
            for h in range(HEADS):
                bias_half[h, r * keys:(r + 1) * keys, :] = (
                    bias_rows[r, h].astype(jnp.float32)[0:keys]
                )

        out_step = max(OUT_STEP, LAG)
        first_out = max(min(FIRST_OUT, chunks - 1 - out_step), 0)
        sum_step = min(out_step + SUM_AFTER, chunks + LAG - first_out)

        @pl.loop(0, chunks + LAG)
        def _(c):
            @pl.when(c + AHEAD < chunks)
            def _():
                relay(c + AHEAD)

            @pl.when(c < chunks)
            def _():
                first_pass(c)

            @pl.when(c >= LAG)
            def _():
                second_pass(c - LAG)

            @pl.when((c >= out_step) & (c < out_step + first_out))
            def _():
                outer_part(c - out_step)

            @pl.when(c == chunks - 1)
            def _():
                pl.loop(first_out, max(chunks - LAG, 0))(outer_part)

            @pl.when(c >= max(chunks, LAG))
            def _():
                outer_part(c - LAG)

            @pl.when((c >= sum_step) & (c < sum_step + first_out))
            def _():
                outer_sum(c - sum_step)

        for r in range(upper):
            for h in range(HEADS):
                part[h // pack, r, h % pack, 0:keys, :] = (
                    bias_sum[h, r * keys:(r + 1) * keys, :].astype(jnp.bfloat16)
                )
        for d in range(1, rows_n):
            peer = lax.rem(row + d, rows_n)
            remote(
                part.at[peer // upper, lax.rem(peer, upper)], part_in.at[row],
                pr_send, pr_recv, (peer, col),
            ).start()
        for n in range(groups):
            own_part(n)
        last_sums = max(chunks - LAST_SUMS, first_out)
        pl.loop(first_out, last_sums)(outer_sum)
        pl.semaphore_wait(greets.at[1], 1)
        greet(greets.at[2], (lax.rem(row + upper, rows_n), col))
        pl.semaphore_wait(greets.at[2], 1)

        many = part_in.at[0:rows_n - 1]
        landed(many, pr_recv)
        sums = []
        for hh in range(pack):
            total = part[group, slot, hh].astype(jnp.float32)
            for d in range(1, rows_n):
                total = total + part_in[lax.rem(row + d, rows_n), hh].astype(jnp.float32)
            sums.append(total.astype(jnp.bfloat16))
        for z in range(cols_n):
            packed = jnp.zeros((padded, lanes), jnp.float32)
            for hh in range(pack):
                packed = packed + jnp.dot(
                    sums[hh], pick(z, hh, (count, lanes), 1), preferred_element_type=jnp.float32
                )
            tile[z] = packed.astype(jnp.bfloat16)
        for z in range(cols_n):
            elsewhere = (owner != row) | (col != z)

            @pl.when(elsewhere)
            def _():
                remote(
                    tile.at[z], tile_in.at[group], pc_send, pc_recv.at[group], (owner, z)
                ).start()

        @pl.when(owner == row)
        def _():
            tile_in[group] = tile[col]

        pl.loop(last_sums, chunks)(outer_sum)

        for n in range(groups):
            landed(gq_in.at[own_rows(n), pl.ds(local, width)], own_recv.at[n])

            @pl.loop(n * grouped, (n + 1) * grouped)
            def _(c):
                total = stage_q[rows_of(c), my_block].astype(jnp.float32)
                total = total + gq_in[rows_of(c), pl.ds(local, width)].astype(jnp.float32)
                gq_ref[rows_of(c)] = total.astype(jnp.bfloat16)

        left(part_in.at[0:rows_n - 1], pr_send)

        @pl.when(holder)
        def _():
            left(bias_long, br_send)
            left(tile.at[0:cols_n - 1], pc_send)

        @pl.when(jnp.logical_not(holder))
        def _():
            left(tile, pc_send)

        left(qg.at[:, :, 0:half], mate_send)
        left(both_stats, stats_send)
        left(gq_in, gq_send)
        left(qg.at[0, :, 0:3 * width], kv_send)

    @pl.when(jnp.logical_not(inner))
    def _():
        landed(qg.at[0, :, 0:3 * width], kv_recv)
        left(mask_send, mask_out)
        left(qg.at[:, :, 0:half], outer_send)

    for n in range(packs):
        @pl.when(jnp.logical_not(holder & (group == n)))
        def _():
            landed(tile_in.at[n], pc_recv.at[n])

    @pl.when(jnp.logical_not(holder))
    def _():
        bias_piece.wait_send()

    for p in range(packs):
        for hh in range(pack):
            gb_ref[p * pack + hh] = tile_in[
                p, 0:keys, hh * width:(hh + 1) * width
            ].astype(jnp.float32)


def writer_kernel(*refs):
    count = len(refs) // 2
    sem = refs[-1]
    copies = [
        pltpu.make_async_copy(refs[n], refs[count + n], sem.at[n]) for n in range(count)
    ]
    for copy in copies:
        copy.start()
    for copy in copies:
        copy.wait()


def written(*arrays):
    return pl.pallas_call(
        writer_kernel,
        name="write_grads",
        out_shape=tuple(jax.ShapeDtypeStruct(a.shape, a.dtype) for a in arrays),
        in_specs=[pl.BlockSpec(memory_space=pl.ANY)] * len(arrays),
        out_specs=(pl.BlockSpec(memory_space=pl.ANY),) * len(arrays),
        scratch_shapes=[pltpu.SemaphoreType.DMA((len(arrays),))],
    )(*(pltpu.with_memory_space_constraint(a, pltpu.VMEM) for a in arrays))


def fused(rows_n, query_proj, key_proj, value_proj, pair_bias, pair_mask, grad_out):
    rows, width, channels = query_proj.shape
    keys = pair_bias.shape[2]
    cols_n = 4
    half, count, upper = 2 * width, 4 * width, rows_n // 2
    pack = 1
    while pack * 2 <= HEADS and pack * 2 * width <= 128:
        pack = pack * 2
    packs = HEADS // pack
    padded, lanes = round_up(keys, 16), round_up(pack * width, 128)
    mask_lanes = round_up(rows, 128)
    chunk = 2 if rows % 2 == 0 else 1
    chunks = rows // chunk
    bf16, f32 = jnp.bfloat16, jnp.float32
    anywhere = pl.BlockSpec(memory_space=pl.ANY)
    on_chip = pl.BlockSpec(memory_space=pltpu.VMEM)
    sem = pltpu.SemaphoreType.DMA
    tile_shape = pltpu.VMEM(query_proj.shape, bf16)
    grads = pl.pallas_call(
        functools.partial(split_kernel, rows_n, pack),
        name="triangle_grads",
        out_shape=(
            tile_shape, tile_shape, tile_shape,
            pltpu.VMEM((HEADS, keys, width), f32),
        ),
        in_specs=[anywhere] * 4 + [on_chip] * 2,
        out_specs=(on_chip,) * 4,
        scratch_shapes=[
            pltpu.VMEM((packs, padded, lanes), bf16),
            pltpu.VMEM((cols_n, packs, padded, lanes), bf16),
            pltpu.VMEM((upper, HEADS, padded, count), bf16),
            pltpu.VMEM((HEADS, half, count), f32),
            pltpu.VMEM((width, mask_lanes), bf16),
            pltpu.VMEM((half, mask_lanes), bf16),
            pltpu.VMEM((2, rows, count, channels), bf16),
            pltpu.VMEM((2, rows, half, channels), bf16),
            pltpu.VMEM((LAG + 1, chunk, HEADS, half, count), f32),
            pltpu.VMEM((LAG + 1, chunk, HEADS, half, count), f32),
            pltpu.VMEM((chunks, HEADS, chunk * count), f32),
            pltpu.VMEM((chunks, HEADS, chunk * count), f32),
            pltpu.VMEM((chunks, HEADS, chunk * count), bf16),
            pltpu.VMEM((chunks, HEADS, chunk * count), bf16),
            pltpu.VMEM((chunks, 3, HEADS, chunk * count), bf16),
            pltpu.VMEM((rows, count, channels), bf16),
            pltpu.VMEM((2, rows, half, channels), bf16),
            pltpu.VMEM((rows, width, channels), bf16),
            pltpu.VMEM((rows, half, channels), bf16),
            pltpu.VMEM((HEADS, half, count), f32),
            pltpu.VMEM((packs, upper, pack, padded, count), bf16),
            pltpu.VMEM((rows_n, pack, padded, count), bf16),
            pltpu.VMEM((rows_n, HEADS, padded, count), bf16),
            pltpu.VMEM((cols_n, padded, lanes), bf16),
            pltpu.VMEM((packs, padded, lanes), bf16),
            sem((chunks,)), sem((chunks,)), sem((chunks,)), sem((chunks,)), sem((chunks,)),
            sem((3 if chunks % 3 == 0 else 1,)), sem((16,)), sem((packs,)), pltpu.SemaphoreType.REGULAR((rows_n.bit_length() + 1,)),
        ],
        compiler_params=pltpu.CompilerParams(collective_id=0, has_side_effects=True),
    )(query_proj, key_proj, value_proj, grad_out, jnp.transpose(pair_bias, (0, 2, 1)), pair_mask)
    gq, gk, gv, gb = written(*grads)
    return gq, gk, gv, jnp.transpose(gb, (0, 2, 1))


def choose(rows_n, cols_n):
    def run(*arrays):
        count = arrays[0].shape[1] * cols_n
        small = count * count * 4 <= 512 * 1024 and arrays[0].shape[0] <= 128
        width = arrays[0].shape[1]
        paired = HEADS == 4 and 32 < width <= 64 and rows_n > 1 and rows_n & (rows_n - 1) == 0
        if small and cols_n == 4 and paired and width % 16 == 0:
            return fused(rows_n, *arrays)
        return local(*arrays)

    return run


def solution(mesh):
    placed = (
        P("row", "col", None),
        P("row", "col", None),
        P("row", "col", None),
        P(None, "col", "row"),
        P("row", "col"),
        P("row", "col", None),
    )
    return jax.shard_map(
        choose(mesh.shape["row"], mesh.shape["col"]),
        mesh=mesh,
        in_specs=placed,
        out_specs=(
            P("row", "col", None),
            P("row", "col", None),
            P("row", "col", None),
            P(None, "col", "row"),
        ),
        check_vma=False,
    )
```
